32 devices in a mesh: feat: 8 (over z, y), samp: 4 (over x, core).
Axes of the slice: x: 2, y: 2, z: 4, core: 2. Of those that a mesh axis runs over, the one named last changes fastest.
Arguments:
- design: bfloat16 [14336, 8192], P('samp', 'feat'), may hold values from -0.0625 to 0.0625
- targets: bfloat16 [14336, 128], P('samp'), may hold values from -26 to 26
- warm_start: float32 [8192, 128], P('feat'), may hold values from -0.6 to 0.6
- active_mask: int32 [2, 8192], P(None, 'feat'), may hold values 0 or 1
- penalty_index: int32 [1], replicated, may hold values from 0 to 7
Outputs:
- coefficients: float32 [8192, 128], P('feat')
- correlations: float32 [3, 8192], P(None, 'feat')
- relative_gaps: float32 [3], replicated
- pruned_counts: float32 [2], replicated
The draws below stay inside these ranges and needn't reach their ends.
All inputs are finite; a program needn't handle non-finite values. No bound on the sum of `active_mask` on one device may be relied on, other than what follows from the above.
Results may differ from the reference program's by a relative error of at most 0.0024.
The reference program's roundings to bfloat16 on the way count: a program that leaves them out, or rounds other values in their place, can miss the bound.
Values may be sent and summed in bfloat16 or wider, within the bound.
A program may use at most 64 MiB of HBM per device.

```python
import jax
import jax.numpy as jnp
from jax import lax

K = 128
ITERS = 2
NS = 14336
P_SIZE = 8192


def draw_targets(key, part):
    phase_key = jax.random.fold_in(key, 11)
    rough_key = jax.random.fold_in(key, 12)
    noise_key = jax.random.fold_in(key, 13)
    positions = jnp.arange(NS).astype(jnp.float32) / NS
    phase = jax.random.uniform(phase_key, (), jnp.float32, 0.0, 6.2831853)
    profile = jnp.exp(1.5 * jnp.sin(6.2831853 * 3.0 * positions + phase))
    rough = jax.random.uniform(rough_key, (NS, 1), jnp.float32, 0.7, 1.4)
    noise = jnp.clip(jax.random.normal(noise_key, (NS, K), jnp.float32), -4.0, 4.0)
    return (noise * profile[:, None] * rough).astype(jnp.bfloat16)


def plant(drawn, key, smallest, top_value):
    extent = drawn.shape
    index_at = [jax.random.randint(jax.random.fold_in(key, axis), (), 0, extent[axis]) for axis in range(len(extent))]
    drawn = drawn.at[tuple(index_at)].set(smallest)
    longest = extent.index(max(extent))
    index_at[longest] = (index_at[longest] + 1) % extent[longest]
    return drawn.at[tuple(index_at)].set(top_value)


def with_spikes(values, own_key, source, target, parts, factor):
    owner, partner = [(jnp.arange(values.shape[axis_at]) // (values.shape[axis_at] // parts)).reshape([-1 if axis == axis_at else 1 for axis in range(values.ndim)]) for axis_at in (source, target)]
    chosen = jax.random.permutation(own_key, parts)[partner]
    strong = (owner == chosen) | (owner == (partner + parts // 2) % parts)
    return jnp.where(strong, factor * values, values)


def levels(rng, extent, pieces, least, high):
    loudness, own = 1.0, jax.random.fold_in(rng, 6)
    for dim, blocks in pieces:
        steps = jnp.exp(jax.random.uniform(jax.random.fold_in(own, dim), (blocks,), jnp.float32, least / len(pieces), high / len(pieces)))
        loudness = loudness * jnp.repeat(steps, extent[dim] // blocks).reshape([-1 if axis == dim else 1 for axis in range(len(extent))])
    return loudness


def scatter_about(stream_key, extent, scale, reach, cuts=(), held_as=jnp.bfloat16):
    drawn = jax.random.normal(stream_key, extent, jnp.float32) * scale
    if len(cuts) > 0:
        drawn = levels(stream_key, extent, cuts, -0.22, 0.18) * drawn
    return jnp.clip(drawn, min=-reach, max=reach).astype(held_as)


def gaussian_with(stream_key, shape, spread, bound, shards, heavy, kind=jnp.bfloat16):
    result = spread * jax.random.normal(stream_key, shape, jnp.float32)
    if shards:
        result = result * levels(stream_key, shape, shards, -0.22, 0.18)
    return jnp.clip(with_spikes(result, jax.random.fold_in(stream_key, 3), *heavy), -bound, bound).astype(kind)


def setup_inputs(seed: int = 0) -> dict:
    key_list = jax.random.split(jax.random.key(seed), 6)
    design = gaussian_with(key_list[0], (NS, P_SIZE), NS ** -0.5, 0.0625, ((0, 4), (1, 8)), (1, 0, 8, 2.0))
    targets = draw_targets(jax.random.fold_in(key_list[5], 71), 0)
    warm_start = scatter_about(key_list[2], (P_SIZE, K), 0.1, 0.6, ((0, 8),), jnp.float32)
    active_mask = plant((jax.random.randint(key_list[3], (ITERS, P_SIZE), 0, 4) < 3).astype(jnp.int32), jax.random.fold_in(key_list[3], 1), 0, 1)
    penalty_index = jax.random.randint(key_list[4], (1,), 0, 8).astype(jnp.int32)
    return {"design": design, "targets": targets, "warm_start": warm_start, "active_mask": active_mask, "penalty_index": penalty_index}


def group_norms(matrix):
    return jnp.sqrt(lax.optimization_barrier(jnp.sum(matrix * matrix, axis=1)))

def transpose_product(design, right_side):
    return lax.dot_general(design, right_side, (((0,), (0,)), ((), ())), preferred_element_type=jnp.float32)

def reference(design, targets, warm_start, active_mask, penalty_index):
    corr_y = transpose_product(design, targets)
    column_squares = lax.optimization_barrier(jnp.sum(jnp.square(design.astype(jnp.float32)), axis=0))
    penalty_max = jnp.max(group_norms(corr_y))
    penalty = penalty_max / (8.0 + 4.0 * penalty_index[0].astype(jnp.float32))
    step_sizes = 0.5 / (1.0 + column_squares)
    target_float = targets.astype(jnp.float32)
    current = warm_start
    correlations = []
    relative_gaps = []
    pruned_counts = []
    for iteration in range(ITERS + 1):
        current_half = current.astype(jnp.bfloat16)
        fitted = jnp.dot(design, current_half, preferred_element_type=jnp.float32)
        residual = (target_float - fitted).astype(jnp.bfloat16)
        resid_float = residual.astype(jnp.float32)
        rr_sum = jnp.sum(resid_float * resid_float)
        ry_sum = jnp.sum(resid_float * target_float)
        bn_sum = jnp.sum(group_norms(current))
        gradient = transpose_product(design, residual)
        grad_norms = group_norms(gradient)
        scale = jnp.maximum(penalty, jnp.max(grad_norms))
        correlations.append(grad_norms / scale)
        primal = 0.5 * rr_sum + penalty * bn_sum
        ratio = penalty / scale
        dual = ratio * ry_sum - 0.5 * ratio * ratio * rr_sum
        relative_gaps.append((primal - dual) / (primal + 1.0))
        if iteration < ITERS:
            keep = active_mask[iteration].astype(jnp.float32)
            pruned_counts.append(jnp.sum(1.0 - keep))
            moved = current + step_sizes[:, None] * gradient
            moved_norms = group_norms(moved)
            cutoff = step_sizes * penalty
            factor = jnp.maximum(moved_norms - cutoff, 0.0) / jnp.maximum(moved_norms, cutoff)
            current = (keep * factor)[:, None] * moved
    return (current, jnp.stack(correlations), jnp.stack(relative_gaps), jnp.stack(pruned_counts))
```

```python
import functools

import jax
import jax.numpy as jnp
from jax import lax
from jax.experimental import pallas as pl
from jax.experimental.pallas import tpu as pltpu
from jax.sharding import PartitionSpec as P

ITERS = 2
F32 = jnp.float32
BF16 = jnp.bfloat16
LANES = 128
SHARE = BF16
GRAD = F32
STATS = 16


def fold(row, combine):
    pieces = [row[:, at : at + LANES] for at in range(0, row.shape[1], LANES)]
    return functools.reduce(combine, pieces)


def top(matrix):
    return jnp.max(jnp.max(matrix, axis=0, keepdims=True), axis=1, keepdims=True)


def total_of(matrix):
    return jnp.sum(jnp.sum(matrix, axis=0, keepdims=True), axis=1, keepdims=True)


def column_norms(matrix):
    return jnp.sqrt(jnp.sum(matrix * matrix, axis=0, keepdims=True))


def kernel(
    sizes, design, targets, warm, mask, index, coef_out, corr_out, info_out,
    mine, ysend, yrecv, zsend, zrecv, resid, turned, gsend, grecv, half, cur, squares,
    sqrecv, coefs, norms, exf, exs,
    y_s, y_r, z_s, z_r, a_s, a_r, b_s, b_r, g_s, g_r, h_s, h_r, q_s, q_r, c_s, c_r, n_s, n_r,
    ef_s, ef_r, es_s, es_r,
):
    F, Z, S = sizes
    R, C = design.shape
    K = targets.shape[1]
    B = R // F
    W = C // S
    f = lax.axis_index("feat")
    s = lax.axis_index("samp")
    z, y = f // 2, lax.rem(f, 2)
    partner = z * 2 + 1 - y

    def ahead_z(off):
        return lax.rem(z + off, Z)

    def behind_z(off):
        return lax.rem(z - off + Z, Z)

    def ahead_s(off):
        return lax.rem(s + off, S)

    def feat_copy(src, dst, send, recv, to):
        return pltpu.make_async_remote_copy(
            src_ref=src, dst_ref=dst, send_sem=send, recv_sem=recv,
            device_id={"feat": to}, device_id_type=pl.DeviceIdType.MESH,
        )

    def samp_copy(src, dst, send, recv, off):
        return pltpu.make_async_remote_copy(
            src_ref=src, dst_ref=dst, send_sem=send, recv_sem=recv,
            device_id={"samp": ahead_s(off)}, device_id_type=pl.DeviceIdType.MESH,
        )

    def copy_y(t, off):
        return feat_copy(ysend.at[t, off], yrecv.at[t, off], y_s.at[t, off], y_r.at[t, off], partner)

    def copy_z(t, off):
        return feat_copy(
            zsend.at[t, off], zrecv.at[t, off], z_s.at[t, off], z_r.at[t, off], ahead_z(off) * 2 + y
        )

    def copy_a(t, off):
        return feat_copy(
            resid.at[t, f], resid.at[t, f], a_s.at[t, off], a_r.at[t, off], ahead_z(off) * 2 + y
        )

    def copy_b(t, off):
        slot = behind_z(off) * 2 + y
        return feat_copy(resid.at[t, slot], resid.at[t, slot], b_s.at[t, off], b_r.at[t, off], partner)

    def copy_g(t, off):
        return samp_copy(gsend.at[t, off], grecv.at[t, off], g_s.at[t, off], g_r.at[t, off], off)

    def copy_h(t, off):
        return samp_copy(half.at[t, s], half.at[t, s], h_s.at[t, off], h_r.at[t, off], off)

    def copy_q(off):
        return samp_copy(squares.at[ahead_s(off)], sqrecv.at[off], q_s.at[off], q_r.at[off], off)

    def copy_c(off):
        return samp_copy(coefs.at[s], coefs.at[s], c_s.at[off], c_r.at[off], off)

    def copy_n(off):
        return samp_copy(norms.at[s], norms.at[s], n_s.at[off], n_r.at[off], off)

    def copy_ef(e, off):
        return feat_copy(
            exf.at[e, f], exf.at[e, f], ef_s.at[e, off], ef_r.at[e, off], lax.rem(f + off, F)
        )

    def copy_es(e, off):
        return samp_copy(exs.at[e, s], exs.at[e, s], es_s.at[e, off], es_r.at[e, off], off)

    def each(count, body, first=0):
        def step(at, carry):
            body(at)
            return carry

        lax.fori_loop(first, count, step, 0)

    barrier = pltpu.get_barrier_semaphore()
    for off in range(1, F):
        pl.semaphore_signal(
            barrier, inc=1, device_id={"feat": lax.rem(f + off, F)}, device_id_type=pl.DeviceIdType.MESH
        )
    for off in range(1, S):
        pl.semaphore_signal(
            barrier, inc=1, device_id={"samp": ahead_s(off)}, device_id_type=pl.DeviceIdType.MESH
        )

    half[0] = warm[...].astype(BF16).reshape(S, W, K)
    norms[s] = jnp.zeros((8, W), F32)
    cur[...] = warm[pl.ds(pl.multiple_of(s * W, W), W), :].T
    pl.semaphore_wait(barrier, F - 1 + S - 1)

    def rows_of(slot):
        return pl.ds(pl.multiple_of(slot * B, B), B)

    def share(t, slot):
        return jnp.dot(design[rows_of(slot), :], half[t].reshape(C, K), preferred_element_type=F32)

    def turn(source):
        step = 2 * B
        for k in range(Z):
            turned[:, k * step : (k + 1) * step] = source(k).T

    def grad_parts(t):
        def part(off):
            at = pl.ds(pl.multiple_of(ahead_s(off) * W, W), W)
            return jnp.dot(turned[...], design[:, at], preferred_element_type=F32)

        def send(off):
            gsend[t, off] = part(off).astype(GRAD)
            copy_g(t, off).start()

        each(S, send, 1)
        gsend_own = part(0)
        return gsend_own

    def grad_sum(t, own):
        for off in range(1, S):
            copy_g(t, off).wait_recv()
            own = own + grecv[t, off].astype(F32)
        return own

    def square_columns():
        tall = 16

        def body(at, acc):
            rows = design[pl.ds(pl.multiple_of(at * tall, tall), tall), :].astype(F32)
            rows = rows * rows
            return acc + rows[:8] + rows[8:]

        acc = lax.fori_loop(0, R // tall, body, jnp.zeros((8, C), F32), unroll=4)
        for c in range(S):
            squares[c] = acc[:, c * W : (c + 1) * W]
        for off in range(1, S):
            copy_q(off).start()

    sums = []
    bn_rows, gmax_rows, pruned_rows = [], [], []
    penalty = None
    step_sizes = None
    for t in range(ITERS + 1):
        bn_rows.append(fold(column_norms(cur[...]), jnp.add))

        def send_y(i):
            off = lax.rem(i + 1, Z)
            ysend[t, off] = share(t, ahead_z(off) * 2 + 1 - y).astype(SHARE)
            copy_y(t, off).start()

        each(Z, send_y)

        def send_z(off):
            mine[...] = share(t, ahead_z(off) * 2 + y)
            copy_y(t, off).wait_recv()
            zsend[t, off] = (mine[...] + yrecv[t, off].astype(F32)).astype(SHARE)
            copy_z(t, off).start()

        each(Z, send_z, 1)
        mine[...] = share(t, f)
        if t == 0:
            turn(lambda k: targets[k * 2 * B : (k + 1) * 2 * B, :])
            corr_own = grad_parts(ITERS + 1)
            square_columns()
        copy_y(t, 0).wait_recv()
        fitted = mine[...] + yrecv[t, 0].astype(F32)
        for off in range(1, Z):
            copy_z(t, off).wait_recv()
            fitted = fitted + zrecv[t, off].astype(F32)
        own_targets = targets[rows_of(f), :].astype(F32)
        rounded = (own_targets - fitted).astype(BF16)
        resid[t, f] = rounded
        for off in range(1, Z):
            copy_a(t, off).start()
        copy_b(t, 0).start()
        wide = rounded.astype(F32)
        sums.append(
            (
                jnp.sum(wide * wide, axis=0, keepdims=True),
                jnp.sum(wide * own_targets, axis=0, keepdims=True),
            )
        )
        if t == 0:
            corr = grad_sum(ITERS + 1, corr_own)
            exf[0, f] = jnp.broadcast_to(fold(column_norms(corr), jnp.maximum), (STATS, LANES))
            for off in range(1, F):
                copy_ef(0, off).start()
            square = squares[s]
            for off in range(1, S):
                copy_q(off).wait_recv()
                square = square + sqrecv[off]
            step_sizes = 0.5 / (1.0 + jnp.sum(square, axis=0, keepdims=True))
        for off in range(1, Z):
            copy_a(t, off).wait_recv()
            copy_b(t, off).start()
        if t == 0:
            for off in range(1, F):
                copy_ef(0, off).wait_recv()
            exs[0, s] = functools.reduce(jnp.maximum, [exf[0, at] for at in range(F)])
            for off in range(1, S):
                copy_es(0, off).start()
        for off in range(Z):
            copy_b(t, off).wait_recv()
        turn(lambda k: resid[t, 2 * k : 2 * k + 2].reshape(2 * B, K))
        own = grad_parts(t)
        gradient = grad_sum(t, own)
        if t == 0:
            for off in range(1, S):
                copy_es(0, off).wait_recv()
            penalty_max = top(functools.reduce(jnp.maximum, [exs[0, at] for at in range(S)]))
            penalty = penalty_max / (8.0 + 4.0 * index[0].astype(F32))
        grad_norms = column_norms(gradient)
        norms[s, t : t + 1, :] = grad_norms
        gmax_rows.append(fold(grad_norms, jnp.maximum))
        if t < ITERS:
            keep = mask[t : t + 1, pl.ds(pl.multiple_of(s * W, W), W)].astype(F32)
            pruned_rows.append(fold(1.0 - keep, jnp.add))
            moved = cur[...] + step_sizes * gradient
            moved_norms = column_norms(moved)
            cutoff = step_sizes * penalty
            factor = jnp.maximum(moved_norms - cutoff, 0.0) / jnp.maximum(moved_norms, cutoff)
            after = (keep * factor) * moved
            cur[...] = after
            upright = after.T
            half[t + 1, s] = upright.astype(BF16)
            for off in range(1, S):
                copy_h(t + 1, off).start()
            if t + 1 == ITERS:
                coefs[s] = upright
                for off in range(1, S):
                    copy_c(off).start()
            for off in range(1, S):
                copy_h(t + 1, off).wait_recv()

    for off in range(1, S):
        copy_n(off).start()
    added = [row[0] for row in sums] + [row[1] for row in sums] + bn_rows + pruned_rows
    n_add = len(added)
    blank = jnp.zeros((STATS - n_add - len(gmax_rows), LANES), F32)
    exf[1, f] = jnp.concatenate(added + gmax_rows + [blank], axis=0)
    for off in range(1, F):
        copy_ef(1, off).start()

    def merge(tiles):
        plus = functools.reduce(jnp.add, tiles)
        most = functools.reduce(jnp.maximum, tiles)
        at = lax.broadcasted_iota(jnp.int32, plus.shape, 0)
        return jnp.where(at < n_add, plus, most)

    for off in range(1, F):
        copy_ef(1, off).wait_recv()
    exs[1, s] = merge([exf[1, at] for at in range(F)])
    for off in range(1, S):
        copy_es(1, off).start()
    for off in range(1, S):
        copy_c(off).wait_recv()
    coef_out[...] = coefs[...].reshape(C, K)
    for off in range(1, S):
        copy_n(off).wait_recv()
    for off in range(1, S):
        copy_es(1, off).wait_recv()
    merged = merge([exs[1, at] for at in range(S)])
    added_up = jnp.sum(merged, axis=1, keepdims=True)
    highest = jnp.max(merged, axis=1, keepdims=True)
    T = ITERS + 1
    lines = []
    for t in range(T):
        rr, ry, bn = (added_up[at : at + 1] for at in (t, T + t, 2 * T + t))
        scale = jnp.maximum(penalty, highest[n_add + t : n_add + t + 1])
        primal = 0.5 * rr + penalty * bn
        ratio = penalty / scale
        dual = ratio * ry - 0.5 * ratio * ratio * rr
        lines.append((primal - dual) / (primal + 1.0))
        for c in range(S):
            corr_out[t : t + 1, c * W : (c + 1) * W] = norms[c, t : t + 1, :] / scale
    for t in range(ITERS):
        lines.append(added_up[3 * T + t : 3 * T + t + 1])
    for at, line in enumerate(lines):
        info_out[at : at + 1, :] = jnp.broadcast_to(line, (1, LANES))

    for t in range(ITERS + 1):
        for off in range(Z):
            copy_y(t, off).wait_send()
            copy_b(t, off).wait_send()
            if off:
                copy_z(t, off).wait_send()
                copy_a(t, off).wait_send()
    for off in range(1, S):
        for t in range(ITERS + 2):
            copy_g(t, off).wait_send()
        for t in range(1, ITERS + 1):
            copy_h(t, off).wait_send()
        copy_q(off).wait_send()
        copy_c(off).wait_send()
        copy_n(off).wait_send()
        copy_es(0, off).wait_send()
        copy_es(1, off).wait_send()
    for off in range(1, F):
        copy_ef(0, off).wait_send()
        copy_ef(1, off).wait_send()


def fused(design, targets, warm_start, active_mask, penalty_index):
    F, S = lax.axis_size("feat"), lax.axis_size("samp")
    R, C = design.shape
    K = targets.shape[1]
    Z, B, W, T = F // 2, R // F, C // S, ITERS + 1
    dma = pltpu.SemaphoreType.DMA
    vmem = pl.BlockSpec(memory_space=pltpu.VMEM)
    coefficients, correlations, info = pl.pallas_call(
        functools.partial(kernel, (F, Z, S)),
        out_shape=(
            jax.ShapeDtypeStruct((C, K), F32),
            jax.ShapeDtypeStruct((T, C), F32),
            jax.ShapeDtypeStruct((8, LANES), F32),
        ),
        in_specs=[vmem] * 4 + [pl.BlockSpec(memory_space=pltpu.SMEM)],
        out_specs=(vmem,) * 3,
        scratch_shapes=[
            pltpu.VMEM((B, K), F32),
            pltpu.VMEM((T, Z, B, K), SHARE),
            pltpu.VMEM((T, Z, B, K), SHARE),
            pltpu.VMEM((T, Z, B, K), SHARE),
            pltpu.VMEM((T, Z, B, K), SHARE),
            pltpu.VMEM((T, F, B, K), BF16),
            pltpu.VMEM((K, R), BF16),
            pltpu.VMEM((T + 1, S, K, W), GRAD),
            pltpu.VMEM((T + 1, S, K, W), GRAD),
            pltpu.VMEM((T, S, W, K), BF16),
            pltpu.VMEM((K, W), F32),
            pltpu.VMEM((S, 8, W), F32),
            pltpu.VMEM((S, 8, W), F32),
            pltpu.VMEM((S, W, K), F32),
            pltpu.VMEM((S, 8, W), F32),
            pltpu.VMEM((2, F, STATS, LANES), F32),
            pltpu.VMEM((2, S, STATS, LANES), F32),
        ]
        + [dma((T, Z))] * 8
        + [dma((T + 1, S))] * 2
        + [dma((T, S))] * 2
        + [dma((S,))] * 6
        + [dma((2, F))] * 2
        + [dma((2, S))] * 2,
        compiler_params=pltpu.CompilerParams(
            collective_id=0, has_side_effects=True, vmem_limit_bytes=62 * 1024 * 1024
        ),
    )(design, targets, warm_start, active_mask, penalty_index)
    gaps = info[: T, 0]
    pruned = info[T : T + ITERS, 0]
    return coefficients, correlations, gaps, pruned


def group_norms(matrix):
    return jnp.sqrt(jnp.sum(matrix * matrix, axis=1))


def transpose_product(design, right_side):
    return lax.dot_general(
        design, right_side, (((0,), (0,)), ((), ())), preferred_element_type=jnp.float32
    )


def plain(design, targets, warm_start, active_mask, penalty_index):
    row_count, col_count = design.shape
    feat_size = lax.axis_size("feat")
    feat_slot = lax.axis_index("feat")
    block_rows = row_count // feat_size
    samp_first = (lax.axis_index("samp") == 0).astype(jnp.float32)
    corr_local = transpose_product(design, targets)
    squares_local = jnp.sum(jnp.square(design.astype(jnp.float32)), axis=0)
    corr_y, column_squares = lax.psum((corr_local, squares_local), "samp")
    penalty_max = lax.pmax(jnp.max(group_norms(corr_y)), "feat")
    penalty = penalty_max / (8.0 + 4.0 * penalty_index[0].astype(jnp.float32))
    step_sizes = 0.5 / (1.0 + column_squares)
    current = warm_start
    correlations = []
    relative_gaps = []
    pruned_counts = []
    own_targets = lax.dynamic_slice_in_dim(targets, feat_slot * block_rows, block_rows, 0)
    for iteration in range(ITERS + 1):
        current_half = current.astype(jnp.bfloat16)
        fitted_part = jnp.dot(design, current_half, preferred_element_type=jnp.float32)
        fitted = lax.psum(fitted_part, "feat")
        residual_all = (targets.astype(jnp.float32) - fitted).astype(jnp.bfloat16)
        residual = lax.dynamic_slice_in_dim(residual_all, feat_slot * block_rows, block_rows, 0)
        grad_local = transpose_product(design, residual_all)
        resid_float = residual.astype(jnp.float32)
        rr_local = jnp.sum(resid_float * resid_float)
        ry_local = jnp.sum(resid_float * own_targets.astype(jnp.float32))
        bn_local = samp_first * jnp.sum(group_norms(current))
        if iteration < ITERS:
            keep = active_mask[iteration].astype(jnp.float32)
            pruned_local = samp_first * jnp.sum(1.0 - keep)
        else:
            pruned_local = jnp.zeros((), jnp.float32)
        gradient = lax.psum(grad_local, "samp")
        grad_norms = group_norms(gradient)
        local_max = jnp.max(grad_norms)
        grad_top = lax.pmax(local_max, "feat")
        rr_sum, ry_sum, bn_sum, pruned_sum = lax.psum(
            (rr_local, ry_local, bn_local, pruned_local), ("feat", "samp")
        )
        scale = jnp.maximum(penalty, grad_top)
        correlations.append(grad_norms / scale)
        primal = 0.5 * rr_sum + penalty * bn_sum
        ratio = penalty / scale
        dual = ratio * ry_sum - 0.5 * ratio * ratio * rr_sum
        relative_gaps.append((primal - dual) / (primal + 1.0))
        if iteration < ITERS:
            pruned_counts.append(pruned_sum)
            moved = current + step_sizes[:, None] * gradient
            moved_norms = group_norms(moved)
            cutoff = step_sizes * penalty
            factor = jnp.maximum(moved_norms - cutoff, 0.0) / jnp.maximum(moved_norms, cutoff)
            current = (keep * factor)[:, None] * moved
    return (current, jnp.stack(correlations), jnp.stack(relative_gaps), jnp.stack(pruned_counts))


def local(design, targets, warm_start, active_mask, penalty_index):
    feat, samp = lax.axis_size("feat"), lax.axis_size("samp")
    rows, cols = design.shape
    fits = (
        feat % 2 == 0
        and rows % (feat * 16) == 0
        and (2 * rows // feat) % LANES == 0
        and cols % (samp * LANES) == 0
        and targets.shape[1] == LANES
    )
    form = fused if fits else plain
    return form(design, targets, warm_start, active_mask, penalty_index)


def solution(mesh):
    placed = (P("samp", "feat"), P("samp", None), P("feat", None), P(None, "feat"), P())
    return jax.shard_map(
        local,
        mesh=mesh,
        in_specs=placed,
        out_specs=(P("feat", None), P(None, "feat"), P(), P()),
        check_vma=False,
    )
```

```python
import functools

import jax
import jax.numpy as jnp
from jax import lax
from jax.experimental import pallas as pl
from jax.experimental.pallas import tpu as pltpu
from jax.sharding import PartitionSpec as P

ITERS = 2
F32 = jnp.float32
BF16 = jnp.bfloat16
LANES = 128
SHARE = BF16
GRAD = BF16
H = 2
STATS = 16


def fold(row, combine):
    pieces = [row[:, at : at + LANES] for at in range(0, row.shape[1], LANES)]
    return functools.reduce(combine, pieces)


def top(matrix):
    return jnp.max(jnp.max(matrix, axis=0, keepdims=True), axis=1, keepdims=True)


def total_of(matrix):
    return jnp.sum(jnp.sum(matrix, axis=0, keepdims=True), axis=1, keepdims=True)


def column_norms(matrix):
    return jnp.sqrt(jnp.sum(matrix * matrix, axis=0, keepdims=True))


def kernel(
    sizes, stored, targets, warm, mask, index, coef_out, corr_out, info_out,
    design, gacc, mine, ysend, yrecv, zsend, zrecv, resid, turned, gsend, grecv, half, cur, squares,
    sqrecv, coefs, norms, exf, exs,
    y_s, y_r, z_s, z_r, a_s, a_r, b_s, b_r, g_s, g_r, h_s, h_r, q_s, q_r, c_s, c_r, n_s, n_r,
    ef_s, ef_r, es_s, es_r, d_s,
):
    F, Z, S = sizes
    R, C = design.shape
    K = targets.shape[1]
    B = R // F
    W = C // S
    b = B // H
    f = lax.axis_index("feat")
    s = lax.axis_index("samp")
    z, y = f // 2, lax.rem(f, 2)
    partner = z * 2 + 1 - y

    def ahead_z(off):
        return lax.rem(z + off, Z)

    def behind_z(off):
        return lax.rem(z - off + Z, Z)

    def ahead_s(off):
        return lax.rem(s + off, S)

    def feat_copy(src, dst, send, recv, to):
        return pltpu.make_async_remote_copy(
            src_ref=src, dst_ref=dst, send_sem=send, recv_sem=recv,
            device_id={"feat": to}, device_id_type=pl.DeviceIdType.MESH,
        )

    def samp_copy(src, dst, send, recv, off):
        return pltpu.make_async_remote_copy(
            src_ref=src, dst_ref=dst, send_sem=send, recv_sem=recv,
            device_id={"samp": ahead_s(off)}, device_id_type=pl.DeviceIdType.MESH,
        )

    def rows_of(slot):
        return pl.ds(pl.multiple_of(slot * B, B), B)

    def half_of(slot, h):
        return pl.ds(pl.multiple_of(slot * B + h * b, b), b)

    def copy_d(own, off):
        at = rows_of(ahead_z(off) * 2 + (y if own else 1 - y))
        return pltpu.make_async_copy(stored.at[at, :], design.at[at, :], d_s.at[own, off])

    def copy_y(t, off, h):
        at = (t, off, h)
        return feat_copy(ysend.at[at], yrecv.at[at], y_s.at[at], y_r.at[at], partner)

    def copy_z(t, off, h):
        at = (t, off, h)
        return feat_copy(zsend.at[at], zrecv.at[at], z_s.at[at], z_r.at[at], ahead_z(off) * 2 + y)

    def copy_a(t, off, h):
        at = (t, off, h)
        own = resid.at[t, f, h]
        return feat_copy(own, own, a_s.at[at], a_r.at[at], ahead_z(off) * 2 + y)

    def copy_b(t, off, h):
        at = (t, off, h)
        block = resid.at[t, behind_z(off) * 2 + y, h]
        return feat_copy(block, block, b_s.at[at], b_r.at[at], partner)

    def copy_g(t, off):
        return samp_copy(gsend.at[t, off], grecv.at[t, off], g_s.at[t, off], g_r.at[t, off], off)

    def copy_h(t, off):
        return samp_copy(half.at[t, s], half.at[t, s], h_s.at[t, off], h_r.at[t, off], off)

    def copy_q(off):
        return samp_copy(squares.at[ahead_s(off)], sqrecv.at[off], q_s.at[off], q_r.at[off], off)

    def copy_c(off):
        return samp_copy(coefs.at[s], coefs.at[s], c_s.at[off], c_r.at[off], off)

    def copy_n(off):
        return samp_copy(norms.at[s], norms.at[s], n_s.at[off], n_r.at[off], off)

    def copy_ef(e, off):
        return feat_copy(
            exf.at[e, f], exf.at[e, f], ef_s.at[e, off], ef_r.at[e, off], lax.rem(f + off, F)
        )

    def copy_es(e, off):
        return samp_copy(exs.at[e, s], exs.at[e, s], es_s.at[e, off], es_r.at[e, off], off)

    def each(count, body, first=0):
        def step(at, carry):
            body(at)
            return carry

        lax.fori_loop(first, count, step, 0)

    for own in range(2):
        for i in range(Z):
            copy_d(own, (i + 1) % Z).start()
    barrier = pltpu.get_barrier_semaphore()
    for off in range(1, F):
        pl.semaphore_signal(
            barrier, inc=1, device_id={"feat": lax.rem(f + off, F)}, device_id_type=pl.DeviceIdType.MESH
        )
    for off in range(1, S):
        pl.semaphore_signal(
            barrier, inc=1, device_id={"samp": ahead_s(off)}, device_id_type=pl.DeviceIdType.MESH
        )

    half[0] = warm[...].astype(BF16).reshape(S, W, K)
    norms[s] = jnp.zeros((8, W), F32)
    cur[...] = warm[pl.ds(pl.multiple_of(s * W, W), W), :].T
    pl.semaphore_wait(barrier, F - 1 + S - 1)

    def share(t, slot, h):
        block = design[half_of(slot, h), :]
        return jnp.dot(block, half[t].reshape(C, K), preferred_element_type=F32)

    def grad_chunk(t, k, chunk, first, last):
        turned[...] = chunk.T
        rows = pl.ds(pl.multiple_of(k * 2 * B, 2 * B), 2 * B)

        def part(off):
            at = pl.ds(pl.multiple_of(ahead_s(off) * W, W), W)
            piece = jnp.dot(turned[...], design[rows, at], preferred_element_type=F32)
            return piece if first else gacc[off] + piece

        def step(off):
            if last:
                gsend[t, off] = part(off).astype(GRAD)
                copy_g(t, off).start()
            else:
                gacc[off] = part(off)

        each(S, step, 1)
        gacc[0] = part(0)

    def grad_sum(t, own):
        for off in range(1, S):
            copy_g(t, off).wait_recv()
            own = own + grecv[t, off].astype(F32)
        return own

    def square_columns():
        tall = 16

        def body(at, acc):
            rows = design[pl.ds(pl.multiple_of(at * tall, tall), tall), :].astype(F32)
            rows = rows * rows
            return acc + rows[:8] + rows[8:]

        acc = lax.fori_loop(0, R // tall, body, jnp.zeros((8, C), F32), unroll=4)
        for c in range(S):
            squares[c] = acc[:, c * W : (c + 1) * W]
        for off in range(1, S):
            copy_q(off).start()

    sums = []
    bn_rows, gmax_rows, pruned_rows = [], [], []
    penalty = None
    step_sizes = None
    for t in range(ITERS + 1):
        bn_rows.append(fold(column_norms(cur[...]), jnp.add))

        for h in range(H):

            def send_y(i):
                off = lax.rem(i + 1, Z)
                if t == 0 and h == 0:
                    copy_d(0, off).wait()
                ysend[t, off, h] = share(t, ahead_z(off) * 2 + 1 - y, h).astype(SHARE)
                copy_y(t, off, h).start()

            each(Z, send_y)

        for h in range(H):

            def send_z(off):
                if t == 0 and h == 0:
                    copy_d(1, off).wait()
                mine[...] = share(t, ahead_z(off) * 2 + y, h)
                copy_y(t, off, h).wait_recv()
                zsend[t, off, h] = (mine[...] + yrecv[t, off, h].astype(F32)).astype(SHARE)
                copy_z(t, off, h).start()

            each(Z, send_z, 1)
        if t == 0:
            copy_d(1, 0).wait()
            for k in range(Z):
                chunk = targets[k * 2 * B : (k + 1) * 2 * B, :]
                grad_chunk(ITERS + 1, k, chunk, k == 0, k == Z - 1)
            corr_own = gacc[0]
            square_columns()
        rr = jnp.zeros((1, K), F32)
        ry = jnp.zeros((1, K), F32)
        for h in range(H):
            fitted = share(t, f, h)
            copy_y(t, 0, h).wait_recv()
            fitted = fitted + yrecv[t, 0, h].astype(F32)
            for off in range(1, Z):
                copy_z(t, off, h).wait_recv()
                fitted = fitted + zrecv[t, off, h].astype(F32)
            own_targets = targets[half_of(f, h), :].astype(F32)
            rounded = (own_targets - fitted).astype(BF16)
            resid[t, f, h] = rounded
            for off in range(1, Z):
                copy_a(t, off, h).start()
            copy_b(t, 0, h).start()
            wide = rounded.astype(F32)
            rr = rr + jnp.sum(wide * wide, axis=0, keepdims=True)
            ry = ry + jnp.sum(wide * own_targets, axis=0, keepdims=True)
        sums.append((rr, ry))
        if t == 0:
            corr = grad_sum(ITERS + 1, corr_own)
            exf[0, f] = jnp.broadcast_to(fold(column_norms(corr), jnp.maximum), (STATS, LANES))
            for off in range(1, F):
                copy_ef(0, off).start()
            square = squares[s]
            for off in range(1, S):
                copy_q(off).wait_recv()
                square = square + sqrecv[off]
            step_sizes = 0.5 / (1.0 + jnp.sum(square, axis=0, keepdims=True))
        if t == 0:
            for off in range(1, F):
                copy_ef(0, off).wait_recv()
            exs[0, s] = functools.reduce(jnp.maximum, [exf[0, at] for at in range(F)])
            for off in range(1, S):
                copy_es(0, off).start()
        for off in range(Z):
            if off + 1 < Z:
                for h in range(H):
                    copy_a(t, off + 1, h).wait_recv()
                    copy_b(t, off + 1, h).start()
            for h in range(H):
                copy_b(t, off, h).wait_recv()
            k = behind_z(off)
            chunk = resid[t, pl.ds(2 * k, 2)].reshape(2 * B, K)
            grad_chunk(t, k, chunk, off == 0, off == Z - 1)
        gradient = grad_sum(t, gacc[0])
        if t == 0:
            for off in range(1, S):
                copy_es(0, off).wait_recv()
            penalty_max = top(functools.reduce(jnp.maximum, [exs[0, at] for at in range(S)]))
            penalty = penalty_max / (8.0 + 4.0 * index[0].astype(F32))
        grad_norms = column_norms(gradient)
        norms[s, t : t + 1, :] = grad_norms
        gmax_rows.append(fold(grad_norms, jnp.maximum))
        if t < ITERS:
            keep = mask[t : t + 1, pl.ds(pl.multiple_of(s * W, W), W)].astype(F32)
            pruned_rows.append(fold(1.0 - keep, jnp.add))
            moved = cur[...] + step_sizes * gradient
            moved_norms = column_norms(moved)
            cutoff = step_sizes * penalty
            factor = jnp.maximum(moved_norms - cutoff, 0.0) / jnp.maximum(moved_norms, cutoff)
            after = (keep * factor) * moved
            cur[...] = after
            upright = after.T
            half[t + 1, s] = upright.astype(BF16)
            for off in range(1, S):
                copy_h(t + 1, off).start()
            if t + 1 == ITERS:
                coefs[s] = upright
                for off in range(1, S):
                    copy_c(off).start()
            for off in range(1, S):
                copy_h(t + 1, off).wait_recv()

    for off in range(1, S):
        copy_n(off).start()
    added = [row[0] for row in sums] + [row[1] for row in sums] + bn_rows + pruned_rows
    n_add = len(added)
    blank = jnp.zeros((STATS - n_add - len(gmax_rows), LANES), F32)
    exf[1, f] = jnp.concatenate(added + gmax_rows + [blank], axis=0)
    for off in range(1, F):
        copy_ef(1, off).start()

    def merge(tiles):
        plus = functools.reduce(jnp.add, tiles)
        most = functools.reduce(jnp.maximum, tiles)
        at = lax.broadcasted_iota(jnp.int32, plus.shape, 0)
        return jnp.where(at < n_add, plus, most)

    for off in range(1, F):
        copy_ef(1, off).wait_recv()
    exs[1, s] = merge([exf[1, at] for at in range(F)])
    for off in range(1, S):
        copy_es(1, off).start()
    for off in range(1, S):
        copy_c(off).wait_recv()
    coef_out[...] = coefs[...].reshape(C, K)
    for off in range(1, S):
        copy_n(off).wait_recv()
    for off in range(1, S):
        copy_es(1, off).wait_recv()
    merged = merge([exs[1, at] for at in range(S)])
    added_up = jnp.sum(merged, axis=1, keepdims=True)
    highest = jnp.max(merged, axis=1, keepdims=True)
    T = ITERS + 1
    lines = []
    for t in range(T):
        rr, ry, bn = (added_up[at : at + 1] for at in (t, T + t, 2 * T + t))
        scale = jnp.maximum(penalty, highest[n_add + t : n_add + t + 1])
        primal = 0.5 * rr + penalty * bn
        ratio = penalty / scale
        dual = ratio * ry - 0.5 * ratio * ratio * rr
        lines.append((primal - dual) / (primal + 1.0))
        for c in range(S):
            corr_out[t : t + 1, c * W : (c + 1) * W] = norms[c, t : t + 1, :] / scale
    for t in range(ITERS):
        lines.append(added_up[3 * T + t : 3 * T + t + 1])
    for at, line in enumerate(lines):
        info_out[at : at + 1, :] = jnp.broadcast_to(line, (1, LANES))

    for t in range(ITERS + 1):
        for h in range(H):

            def drain(off):
                copy_y(t, off, h).wait_send()
                copy_b(t, off, h).wait_send()

            def drain_line(off):
                copy_z(t, off, h).wait_send()
                copy_a(t, off, h).wait_send()

            each(Z, drain)
            each(Z, drain_line, 1)
    for off in range(1, S):
        for t in range(ITERS + 2):
            copy_g(t, off).wait_send()
        for t in range(1, ITERS + 1):
            copy_h(t, off).wait_send()
        copy_q(off).wait_send()
        copy_c(off).wait_send()
        copy_n(off).wait_send()
        copy_es(0, off).wait_send()
        copy_es(1, off).wait_send()
    for off in range(1, F):
        copy_ef(0, off).wait_send()
        copy_ef(1, off).wait_send()


def finish(coef, corr, info, coef_out, corr_out, gaps_out, pruned_out):
    coef_out[...] = coef[...]
    corr_out[...] = corr[...]
    for at in range(ITERS + 1):
        gaps_out[at] = info[at, 0]
    for at in range(ITERS):
        pruned_out[at] = info[ITERS + 1 + at, 0]


def fused(design, targets, warm_start, active_mask, penalty_index):
    F, S = lax.axis_size("feat"), lax.axis_size("samp")
    R, C = design.shape
    K = targets.shape[1]
    Z, B, W, T = F // 2, R // F, C // S, ITERS + 1
    dma = pltpu.SemaphoreType.DMA
    vmem = pl.BlockSpec(memory_space=pltpu.VMEM)
    coefficients, correlations, info = pl.pallas_call(
        functools.partial(kernel, (F, Z, S)),
        out_shape=(
            jax.ShapeDtypeStruct((C, K), F32),
            jax.ShapeDtypeStruct((T, C), F32),
            jax.ShapeDtypeStruct((8, LANES), F32),
        ),
        in_specs=[pl.BlockSpec(memory_space=pl.ANY)] + [vmem] * 3 + [pl.BlockSpec(memory_space=pltpu.SMEM)],
        out_specs=(vmem,) * 3,
        scratch_shapes=[
            pltpu.VMEM((R, C), BF16),
            pltpu.VMEM((S, K, W), F32),
            pltpu.VMEM((B // H, K), F32),
            pltpu.VMEM((T, Z, H, B // H, K), SHARE),
            pltpu.VMEM((T, Z, H, B // H, K), SHARE),
            pltpu.VMEM((T, Z, H, B // H, K), SHARE),
            pltpu.VMEM((T, Z, H, B // H, K), SHARE),
            pltpu.VMEM((T, F, H, B // H, K), BF16),
            pltpu.VMEM((K, 2 * B), BF16),
            pltpu.VMEM((T + 1, S, K, W), GRAD),
            pltpu.VMEM((T + 1, S, K, W), GRAD),
            pltpu.VMEM((T, S, W, K), BF16),
            pltpu.VMEM((K, W), F32),
            pltpu.VMEM((S, 8, W), F32),
            pltpu.VMEM((S, 8, W), F32),
            pltpu.VMEM((S, W, K), F32),
            pltpu.VMEM((S, 8, W), F32),
            pltpu.VMEM((2, F, STATS, LANES), F32),
            pltpu.VMEM((2, S, STATS, LANES), F32),
        ]
        + [dma((T, Z, H))] * 8
        + [dma((T + 1, S))] * 2
        + [dma((T, S))] * 2
        + [dma((S,))] * 6
        + [dma((2, F))] * 2
        + [dma((2, S))] * 2
        + [dma((2, Z))],
        compiler_params=pltpu.CompilerParams(
            collective_id=0, has_side_effects=True, vmem_limit_bytes=62 * 1024 * 1024
        ),
    )(design, targets, warm_start, active_mask, penalty_index)
    smem = pl.BlockSpec(memory_space=pltpu.SMEM)
    return pl.pallas_call(
        finish,
        out_shape=(
            jax.ShapeDtypeStruct((C, K), F32),
            jax.ShapeDtypeStruct((T, C), F32),
            jax.ShapeDtypeStruct((T,), F32),
            jax.ShapeDtypeStruct((ITERS,), F32),
        ),
        in_specs=[vmem, vmem, smem],
        out_specs=(vmem, vmem, smem, smem),
    )(coefficients, correlations, info)


def group_norms(matrix):
    return jnp.sqrt(jnp.sum(matrix * matrix, axis=1))


def transpose_product(design, right_side):
    return lax.dot_general(
        design, right_side, (((0,), (0,)), ((), ())), preferred_element_type=jnp.float32
    )


def plain(design, targets, warm_start, active_mask, penalty_index):
    row_count, col_count = design.shape
    feat_size = lax.axis_size("feat")
    feat_slot = lax.axis_index("feat")
    block_rows = row_count // feat_size
    samp_first = (lax.axis_index("samp") == 0).astype(jnp.float32)
    corr_local = transpose_product(design, targets)
    squares_local = jnp.sum(jnp.square(design.astype(jnp.float32)), axis=0)
    corr_y, column_squares = lax.psum((corr_local, squares_local), "samp")
    penalty_max = lax.pmax(jnp.max(group_norms(corr_y)), "feat")
    penalty = penalty_max / (8.0 + 4.0 * penalty_index[0].astype(jnp.float32))
    step_sizes = 0.5 / (1.0 + column_squares)
    current = warm_start
    correlations = []
    relative_gaps = []
    pruned_counts = []
    own_targets = lax.dynamic_slice_in_dim(targets, feat_slot * block_rows, block_rows, 0)
    for iteration in range(ITERS + 1):
        current_half = current.astype(jnp.bfloat16)
        fitted_part = jnp.dot(design, current_half, preferred_element_type=jnp.float32)
        fitted = lax.psum(fitted_part, "feat")
        residual_all = (targets.astype(jnp.float32) - fitted).astype(jnp.bfloat16)
        residual = lax.dynamic_slice_in_dim(residual_all, feat_slot * block_rows, block_rows, 0)
        grad_local = transpose_product(design, residual_all)
        resid_float = residual.astype(jnp.float32)
        rr_local = jnp.sum(resid_float * resid_float)
        ry_local = jnp.sum(resid_float * own_targets.astype(jnp.float32))
        bn_local = samp_first * jnp.sum(group_norms(current))
        if iteration < ITERS:
            keep = active_mask[iteration].astype(jnp.float32)
            pruned_local = samp_first * jnp.sum(1.0 - keep)
        else:
            pruned_local = jnp.zeros((), jnp.float32)
        gradient = lax.psum(grad_local, "samp")
        grad_norms = group_norms(gradient)
        local_max = jnp.max(grad_norms)
        grad_top = lax.pmax(local_max, "feat")
        rr_sum, ry_sum, bn_sum, pruned_sum = lax.psum(
            (rr_local, ry_local, bn_local, pruned_local), ("feat", "samp")
        )
        scale = jnp.maximum(penalty, grad_top)
        correlations.append(grad_norms / scale)
        primal = 0.5 * rr_sum + penalty * bn_sum
        ratio = penalty / scale
        dual = ratio * ry_sum - 0.5 * ratio * ratio * rr_sum
        relative_gaps.append((primal - dual) / (primal + 1.0))
        if iteration < ITERS:
            pruned_counts.append(pruned_sum)
            moved = current + step_sizes[:, None] * gradient
            moved_norms = group_norms(moved)
            cutoff = step_sizes * penalty
            factor = jnp.maximum(moved_norms - cutoff, 0.0) / jnp.maximum(moved_norms, cutoff)
            current = (keep * factor)[:, None] * moved
    return (current, jnp.stack(correlations), jnp.stack(relative_gaps), jnp.stack(pruned_counts))


def local(design, targets, warm_start, active_mask, penalty_index):
    feat, samp = lax.axis_size("feat"), lax.axis_size("samp")
    rows, cols = design.shape
    fits = (
        feat % 2 == 0
        and rows % (feat * 16 * H) == 0
        and (2 * rows // feat) % LANES == 0
        and cols % (samp * LANES) == 0
        and targets.shape[1] == LANES
    )
    form = fused if fits else plain
    return form(design, targets, warm_start, active_mask, penalty_index)


def solution(mesh):
    placed = (P("samp", "feat"), P("samp", None), P("feat", None), P(None, "feat"), P())
    return jax.shard_map(
        local,
        mesh=mesh,
        in_specs=placed,
        out_specs=(P("feat", None), P(None, "feat"), P(), P()),
        check_vma=False,
    )
```
